512 devices in a mesh: seq: 64 (over z, y_lo, core), head: 8 (over y_hi, x).
Axes of the slice: x: 4, y: 4 (y_hi: 2, y_lo: 2; y = y_hi * 2 + y_lo), z: 16, core: 2. Of those that a mesh axis runs over, the one named last changes fastest.
Arguments:
- q_main: bfloat16 [8192, 128, 576], P('seq', 'head'), may hold values from -6 to 6
- latent_keys: bfloat16 [8192, 576], P('seq'), may hold values from -6 to 6
- lse_main: float32 [8192, 128], P('seq', 'head'), may hold values from 0.5 to 2.5
- index_queries: bfloat16 [8192, 64, 128], P('seq', 'head'), may hold values from -6 to 6
- index_weights: float32 [8192, 64], P('seq', 'head'), may hold values from -1.5 to 1.5
- index_keys: bfloat16 [8192, 128], P('seq'), may hold values from -6 to 6
- lse_index: float32 [8192], P('seq'), may hold values from 0 to 2
- slab_order: int32 [64], replicated, may hold values from 0 to 63, each once
- block_live: int32 [64, 64], replicated, may hold values 0 or 1
Outputs:
- key_grad: float32 [8192, 128], P('seq')
The draws below stay inside these ranges and needn't reach their ends.
Inputs may be any that keep to these rules, and one draw needn't show every extreme that they name: `slab_order`: a permutation: every slab number once.
All inputs are finite; a program needn't handle non-finite values.
Results may differ from the reference program's by a relative error of at most 0.0028.
Values may be sent and summed in bfloat16 or wider, within the bound.
A program may use at most 64 MiB of HBM per device.

```python
import jax
import jax.numpy as jnp
from jax import lax

HEADS = 128
LATENT = 576
IHEADS = 64
IDIM = 128
TOK_DEV = 128
HOPS = 8
TOKENS = 8192
N_SEQ = 64


def plant(array, rng, smallest, high):
    spot = [jax.random.randint(jax.random.fold_in(rng, axis), (), 0, length) for axis, length in enumerate(array.shape)]
    main_axis = array.shape.index(max(array.shape))
    neighbour = spot[:main_axis] + [(spot[main_axis] + 1) % array.shape[main_axis]] + spot[main_axis + 1:]
    return array.at[tuple(spot)].set(smallest).at[tuple(neighbour)].set(high)


def level_of(rng, extent, cuts, low, top_value):
    loudness, own = 1.0, jax.random.fold_in(rng, 6)
    for dim, parts in cuts:
        heights = jnp.exp(jax.random.uniform(jax.random.fold_in(own, dim), (parts,), jnp.float32, low / len(cuts), top_value / len(cuts)))
        loudness = loudness * jnp.repeat(heights, extent[dim] // parts).reshape([-1 if axis == dim else 1 for axis in range(len(extent))])
    return loudness


def noise(key, dims, spread, bound, cuts=(), held_as=jnp.bfloat16):
    entries = jax.random.normal(key, dims, jnp.float32) * spread
    if len(cuts) > 0:
        entries = level_of(key, dims, cuts, -0.22, 0.18) * entries
    return jnp.clip(entries, min=-bound, max=bound).astype(held_as)


def setup_inputs(seed: int = 0) -> dict:
    seeds = jax.random.split(jax.random.key(seed), 10)
    return {
        "q_main": noise(seeds[0], (TOKENS, HEADS, LATENT), 1.0, 6.0, ((0, 64), (1, 8))),
        "latent_keys": noise(seeds[1], (TOKENS, LATENT), 1.0, 6.0, ((0, 64),)),
        "lse_main": jnp.clip(0.5 + 2.0 * jax.random.uniform(seeds[2], (TOKENS, HEADS), jnp.float32) ** level_of(seeds[2], (TOKENS, HEADS), ((0, 64), (1, 8)), -0.2, 0.2), 0.5, 2.5),
        "index_queries": noise(seeds[3], (TOKENS, IHEADS, IDIM), 1.0, 6.0, ((0, 64), (1, 8))),
        "index_weights": noise(seeds[4], (TOKENS, IHEADS), 0.25, 1.5, ((0, 64), (1, 8)), jnp.float32),
        "index_keys": noise(seeds[5], (TOKENS, IDIM), 1.0, 6.0, ((0, 64),)),
        "lse_index": jnp.clip(2.0 * jax.random.uniform(seeds[6], (TOKENS,), jnp.float32) ** level_of(seeds[6], (TOKENS,), ((0, 64),), -0.2, 0.2), 0.0, 2.0),
        "slab_order": jax.random.permutation(seeds[7], N_SEQ).astype(jnp.int32),
        "block_live": plant((jax.random.randint(seeds[8], (N_SEQ, N_SEQ), 0, 4) < 3).astype(jnp.int32), jax.random.fold_in(seeds[8], 1), 0, 1),
    }


main_scale = 1.0 / 192.0 ** 0.5


def reference(q_main, latent_keys, lse_main, index_queries, index_weights, index_keys, lse_index, slab_order, block_live):
    index_scale = 1.0 / IDIM ** 0.5
    within = jnp.arange(TOK_DEV, dtype=jnp.int32)

    def one_block(key_place):
        key_slab = slab_order[key_place]
        key_start = (key_place * TOK_DEV).astype(jnp.int32)
        latent_block = lax.dynamic_slice_in_dim(latent_keys, key_start, TOK_DEV, 0).astype(jnp.float32)
        key_block = lax.dynamic_slice_in_dim(index_keys, key_start, TOK_DEV, 0).astype(jnp.float32)
        key_spots = key_slab * TOK_DEV + within
        key_total = jnp.zeros((TOK_DEV, IDIM), jnp.float32)
        for cycle_step in range(HOPS):
            query_place = ((key_place + cycle_step) % N_SEQ).astype(jnp.int32)
            query_slab = slab_order[query_place]
            query_start = (query_place * TOK_DEV).astype(jnp.int32)
            queries = lax.dynamic_slice_in_dim(q_main, query_start, TOK_DEV, 0).astype(jnp.float32)
            lse_rows = lax.dynamic_slice_in_dim(lse_main, query_start, TOK_DEV, 0)
            index_rows = lax.dynamic_slice_in_dim(index_queries, query_start, TOK_DEV, 0).astype(jnp.float32)
            weight_rows = lax.dynamic_slice_in_dim(index_weights, query_start, TOK_DEV, 0)
            lse_query = lax.dynamic_slice_in_dim(lse_index, query_start, TOK_DEV, 0)
            query_spots = query_slab * TOK_DEV + within
            scores = jnp.einsum("thc,kc->thk", queries, latent_block) * main_scale
            head_mass = jnp.sum(jnp.exp(scores - lse_rows[:, :, None]), axis=1)
            relu_input = jnp.einsum("tjc,kc->tjk", index_rows, key_block) * index_scale
            logits = jnp.sum(weight_rows[:, :, None] * jnp.maximum(relu_input, 0.0), axis=1)
            live_mask = (key_spots[None, :] <= query_spots[:, None]) & (block_live[query_slab, key_slab] == 1)
            grad_tile = jnp.where(live_mask, jnp.exp(logits - lse_query[:, None]) - head_mass / HEADS, 0.0)
            weighted = jnp.where(relu_input > 0.0, grad_tile[:, None, :] * weight_rows[:, :, None], 0.0).astype(jnp.bfloat16)
            summed = jnp.einsum("tjk,tjc->kc", weighted.astype(jnp.float32), index_rows)
            key_total = key_total + summed * index_scale
        return key_total

    blocks = lax.map(one_block, jnp.arange(N_SEQ, dtype=jnp.int32))
    return blocks.reshape(TOKENS, IDIM)
```

```python
import math

import jax
import jax.numpy as jnp
from jax import lax
from jax.experimental import pallas as pl
from jax.experimental.pallas import tpu as pltpu
from jax.sharding import PartitionSpec as P

HEADS = 128
HOPS = 8
NX = 4

MESH = pl.DeviceIdType.MESH
F32 = jnp.float32
BF16 = jnp.bfloat16
MAIN_SCALE = 1.0 / 192.0**0.5
LOG2E = math.log2(math.e)
NT = (((1,), (1,)), ((), ()))


def dot_nt(a, b):
    return lax.dot_general(a, b, NT, preferred_element_type=F32)


def make_kernel(nseq, nh):
    T = 128
    TS = T // nh
    HL = 128 // nh
    JL = 64 // nh
    PR = nh - 1
    HALF, QUART = T // 2, T // 4
    index_scale = 1.0 / 128.0**0.5
    UNROLL = 4
    SLOTS = ((0, 1), (1, 2), (3, 2), (5, 2), (7, 1))

    def kernel(
        q_hbm, lat_hbm, lse_hbm, iq_hbm, iw_hbm, ik_hbm, lsei_hbm, order_hbm, blive_hbm,
        out_ref,
        q, lat_t, kl, ki, lse, iq, iqt, iw, wb, lsei, order, blive, mask, mt,
        m0, m1, m2, m3, m4, r0, r1, r2, r3, r4,
        x0, x1, x2, x3, x4, lg0, lg1, lg2, lg3, lg4, wt,
        g0, g1, g2, g3, g4, h0, h1, h2, h3, h4,
        o0, o1, o2, o3, o4, orecv, fin,
        loc, zs, zr, xs, xr, ds, dr, iqs, iqr, ws, wr, ms, mr, gs, gr, osem, orsem, as_, ar,
    ):
        M = (m0, m1, m2, m3, m4)
        RM = (r0, r1, r2, r3, r4)
        X = (x0, x1, x2, x3, x4)
        LG = (lg0, lg1, lg2, lg3, lg4)
        G = (g0, g1, g2, g3, g4)
        RG = (h0, h1, h2, h3, h4)
        O = (o0, o1, o2, o3, o4)
        d = lax.axis_index("seq")
        h = lax.axis_index("head")
        c = lax.rem(d, 2)
        x = lax.rem(h, NX)
        yh = h - x
        half = pl.multiple_of(HALF * lax.rem(x, 2), HALF)
        quart = pl.multiple_of(half + QUART * (x // 2), QUART)

        def seq(offset):
            return lax.rem(d + offset + nseq, nseq)

        def peer(r):
            return lax.rem(h + r, nh)

        def xpeer(step):
            return yh + lax.rem(x + step, NX)

        barrier = pltpu.get_barrier_semaphore()
        for r in range(1, nh):
            pl.semaphore_signal(barrier, inc=1, device_id=(d, peer(r)), device_id_type=MESH)
        for k in range(1, HOPS):
            pl.semaphore_signal(barrier, inc=1, device_id=(seq(k), h), device_id_type=MESH)
            pl.semaphore_signal(barrier, inc=1, device_id=(seq(-k), h), device_id_type=MESH)

        mine = pl.ds(pl.multiple_of(h * TS, TS), TS)
        my_rows = pl.ds(pl.multiple_of(h * TS * JL, TS * JL), TS * JL)
        locals_ = [
            pltpu.make_async_copy(lat_hbm, lat_t, loc.at[0]),
            pltpu.make_async_copy(q_hbm, q, loc.at[1]),
            pltpu.make_async_copy(lse_hbm, lse, loc.at[2]),
            pltpu.make_async_copy(ik_hbm, ki.at[0], loc.at[3]),
            pltpu.make_async_copy(iq_hbm.at[my_rows, :], iq.at[PR], loc.at[4]),
            pltpu.make_async_copy(iw_hbm, iw.at[PR], loc.at[5]),
            pltpu.make_async_copy(lsei_hbm, lsei, loc.at[6]),
            pltpu.make_async_copy(order_hbm, order, loc.at[7]),
            pltpu.make_async_copy(blive_hbm, blive, loc.at[8]),
        ]
        for cp in locals_:
            cp.start()
        for cp in locals_:
            cp.wait()

        kl[0] = lat_t[...].T
        lse[...] = lse[...] * LOG2E

        pl.semaphore_wait(barrier, PR + 2 * (HOPS - 1))

        def rcopy(src, dst, s, r, dev):
            return pltpu.make_async_remote_copy(
                src_ref=src, dst_ref=dst, send_sem=s, recv_sem=r, device_id=dev, device_id_type=MESH
            )

        def pieces(src_l, src_i, block, rows, s, r, dev):
            return [
                rcopy(src_l.at[rows, :], kl.at[block, rows, :], s.at[0], r.at[0], dev),
                rcopy(src_i.at[rows, :], ki.at[block, rows, :], s.at[1], r.at[1], dev),
            ]

        def kpieces(block, rows, s, r, dev):
            return pieces(kl.at[block], ki.at[block], block, rows, s, r, dev)

        halfrows = pl.ds(half, HALF)
        quartrows = pl.ds(quart, QUART)
        allrows = pl.ds(0, T)

        def zcopies(j):
            if j < 4:
                return pieces(kl.at[0], ki.at[0], 2 * j - 1 + c, halfrows, zs.at[j - 1], zr.at[j - 1], (seq(2 * j), h))
            return pieces(kl.at[0], ki.at[0], 7, halfrows, zs.at[3], zr.at[3], (seq(7), h))

        def own_to_partner():
            return pieces(kl.at[0], ki.at[0], 7, allrows, ds.at[3], dr.at[3], (seq(1), h))

        for cp in zcopies(1):
            cp.start()
        for r in range(1, nh):
            to = peer(r)
            rows = pl.ds(pl.multiple_of(to * TS * JL, TS * JL), TS * JL)
            rcopy(iq_hbm.at[rows, :], iq.at[r - 1], iqs, iqr, (d, to)).start()
            rcopy(iw_hbm, iw.at[r - 1], ws, wr, (d, to)).start()
        for j in (2, 3):
            for cp in zcopies(j):
                cp.start()

        @pl.when(c == 1)
        def _():
            for cp in zcopies(4):
                cp.start()

        @pl.when(c == 0)
        def _():
            for cp in own_to_partner():
                cp.start()

        lane64 = lax.broadcasted_iota(jnp.int32, (1, nseq), 1)
        order_f = order[...].astype(F32)

        def entry(at):
            return jnp.sum(jnp.where(lane64 == at, order_f, 0.0), axis=1, keepdims=True)

        own_slab = entry(d)
        row64 = lax.broadcasted_iota(jnp.int32, (nseq, nseq), 0).astype(F32)
        live_row = jnp.sum(jnp.where(row64 == own_slab, blive[...].astype(F32), 0.0), axis=0, keepdims=True)
        lane64f = lane64.astype(F32)
        t_at = (h * TS + lax.broadcasted_iota(jnp.int32, (TS, T), 0)).astype(F32) + own_slab * T
        s_in = lax.broadcasted_iota(jnp.int32, (TS, T), 1).astype(F32)
        hops = [0 * c] + [2 * j + c - cc for j in (1, 2, 3) for cc in (0, 1)] + [7 - 6 * c]
        for b in range(8):
            slab = entry(seq(-hops[b]))
            allowed = jnp.sum(jnp.where(lane64f == slab, live_row, 0.0), axis=1, keepdims=True)
            mask[b] = jnp.where((s_in + slab * T <= t_at) & (allowed == 1.0), 1.0, 0.0)
        lane_t = lax.broadcasted_iota(jnp.int32, (TS, T), 1)
        row_t = h * TS + lax.broadcasted_iota(jnp.int32, (TS, T), 0)
        lse_col = jnp.sum(jnp.where(lane_t == row_t, lsei[...], 0.0), axis=1, keepdims=True)

        def mass(si):
            b0, nb = SLOTS[si]
            rows = pl.ds(0, nb * T)
            mt[rows, :] = jnp.zeros((nb * T, T), F32)

            @pl.loop(0, HL // (2 * UNROLL))
            def _(i):
                keys = kl[b0 : b0 + nb].reshape(nb * T, 576)
                part = None
                for u in range(UNROLL):
                    h0 = 2 * (i * UNROLL + u)
                    sc = jnp.dot(keys, jnp.concatenate([q[h0], q[h0 + 1]], axis=1), preferred_element_type=F32)
                    for v in range(2):
                        e = jnp.exp2(sc[:, v * T : (v + 1) * T] * (MAIN_SCALE * LOG2E) - lse[pl.ds(h0 + v, 1), :])
                        part = e if part is None else part + e
                mt[rows, :] += part

            for b in range(nb):
                M[si][:, b * T : (b + 1) * T] = mt[b * T : (b + 1) * T, :].T

            for r in range(1, nh):
                to = peer(r)
                toks = pl.ds(pl.multiple_of(to * TS, TS), TS)
                rcopy(M[si].at[toks, :], RM[si].at[r - 1], ms.at[si], mr.at[si], (d, to)).start()

        def wait_all(ref, sem):
            pltpu.make_async_copy(ref, ref, sem).wait()

        def wait_recv(copies):
            for cp in copies:
                cp.wait_recv()

        def z_arrived(j):
            wait_recv(kpieces(2 * j - 1 + c if j < 4 else 7, halfrows, zs.at[j - 1], zr.at[j - 1], (d, h)))

        def x_copies(j, way):
            return kpieces(2 * j - 1 + c if j < 4 else 7, quartrows, xs.at[j - 1, way], xr.at[j - 1, way], (d, xpeer((1, NX - 1)[way])))

        def x_forward(j):
            for way in (0, 1):
                for cp in x_copies(j, way):
                    cp.start()

        def x_arrived(j):
            for way in (0, 1):
                wait_recv(x_copies(j, way))

        def d_copies(j):
            return kpieces(2 * j - 1 + c, allrows, ds.at[j - 1], dr.at[j - 1], (d + 1 - 2 * c, h))

        def d_forward(j):
            for cp in d_copies(j):
                cp.start()

        def relay_z(j):
            z_arrived(j)
            x_forward(j)

        def relay_x(j):
            x_arrived(j)
            d_forward(j)

        def index_tables():
            wait_all(iq.at[0:PR], iqr)
            wait_all(iw.at[0:PR], wr)
            eye = jnp.where(
                lax.broadcasted_iota(jnp.int32, (T, T), 0) == lax.broadcasted_iota(jnp.int32, (T, T), 1), 1.0, 0.0
            ).astype(BF16)
            pick = lax.broadcasted_iota(jnp.int32, (TS, JL, T), 0) + h * TS == lax.broadcasted_iota(jnp.int32, (TS, JL, T), 2)
            for hh in range(nh):
                iqt[:, hh * T : (hh + 1) * T] = dot_nt(eye, iq[hh]).astype(BF16)
                w = jnp.broadcast_to(iw[hh][None], (TS, JL, T))
                col = jnp.sum(jnp.where(pick, w, 0.0), axis=2, keepdims=True).reshape(TS * JL, 1)
                wb[hh] = jnp.broadcast_to(col, (TS * JL, T))

        def wide(v, nb):
            return jnp.concatenate([v] * nb, axis=1) if nb > 1 else v

        def phase_a(si):
            b0, nb = SLOTS[si]
            keys = ki[b0 : b0 + nb].reshape(nb * T, T)
            LG[si][...] = jnp.zeros_like(LG[si])

            @pl.loop(0, nh)
            def _(hh):
                xv = dot_nt(iq[hh], keys)
                X[si][hh] = xv
                LG[si][...] += jnp.sum(
                    (jnp.maximum(xv, 0.0) * wide(wb[hh], nb)).reshape(TS, JL, nb * T), axis=1
                )

        def phase_b(si):
            b0, nb = SLOTS[si]
            wait_all(RM[si], mr.at[si])
            total = M[si][mine, :]
            for r in range(PR):
                total = total + RM[si][r]
            live = jnp.concatenate([mask[b0 + b] for b in range(nb)], axis=1) if nb > 1 else mask[b0]
            g = jnp.where(live > 0.0, jnp.exp(LG[si][...] * index_scale - lse_col) - total * (1.0 / HEADS), 0.0)
            LG[si][...] = g

            @pl.loop(0, nh)
            def _(hh):
                rows = pl.ds(pl.multiple_of(hh * TS * JL, TS * JL), TS * JL)
                gv = jnp.broadcast_to(LG[si][...][:, None, :], (TS, JL, nb * T)).reshape(TS * JL, nb * T)
                wt[rows, 0 : nb * T] = jnp.where(X[si][hh] > 0.0, gv * wide(wb[hh], nb), 0.0).astype(BF16)

            G[si][...] = jnp.dot(iqt[...], wt[:, 0 : nb * T], preferred_element_type=F32)
            for r in range(1, nh):
                to = peer(r)
                toks = pl.ds(pl.multiple_of(to * TS, TS), TS)
                rcopy(G[si].at[toks, :], RG[si].at[r - 1], gs.at[si], gr.at[si], (d, to)).start()

        def phase_c(si):
            b0, nb = SLOTS[si]
            wait_all(RG[si], gr.at[si])
            total = G[si][mine, :]
            for r in range(PR):
                total = total + RG[si][r]
            O[si][...] = total
            if si > 0:
                for b in range(nb):
                    k = hops[b0 + b]
                    rcopy(
                        O[si].at[:, b * T : (b + 1) * T], orecv.at[k - 1], osem, orsem, (seq(-k), h)
                    ).start()

        mass(0)
        relay_z(1)
        relay_z(2)
        relay_x(1)
        relay_z(3)
        index_tables()
        phase_a(0)
        wait_d = lambda j: wait_recv(
            kpieces(2 * j - c, allrows, ds.at[j - 1], dr.at[j - 1], (d, h))
        )
        wait_d(1)
        mass(1)
        phase_a(1)
        relay_x(2)

        @pl.when(c == 0)
        def _():
            relay_z(4)

        wait_d(2)
        mass(2)
        phase_a(2)
        phase_b(0)
        relay_x(3)
        wait_d(3)
        mass(3)
        phase_a(3)
        phase_b(1)

        @pl.when(c == 0)
        def _():
            x_arrived(4)

        @pl.when(c == 1)
        def _():
            wait_recv(own_to_partner())

        mass(4)
        phase_a(4)
        phase_c(0)
        phase_b(2)
        phase_c(1)
        phase_b(3)
        phase_c(2)
        phase_b(4)
        phase_c(3)
        phase_c(4)

        wait_all(orecv, orsem)
        total = O[0][...]
        for k in range(HOPS - 1):
            total = total + orecv[k]
        fin[mine, :] = total * index_scale
        for r in range(1, nh):
            rcopy(fin.at[mine, :], fin.at[mine, :], as_, ar, (d, peer(r))).start()
        wait_all(orecv, ar) if TS * PR * T == (HOPS - 1) * TS * T else None
        out_ref[...] = fin[...].T

        for j in (1, 2, 3):
            for cp in zcopies(j) + x_copies(j, 0) + x_copies(j, 1) + d_copies(j):
                cp.wait_send()

        @pl.when(c == 1)
        def _():
            for cp in zcopies(4):
                cp.wait_send()

        @pl.when(c == 0)
        def _():
            for cp in own_to_partner() + x_copies(4, 0) + x_copies(4, 1):
                cp.wait_send()

        wait_all(iq.at[0:PR], iqs)
        wait_all(iw.at[0:PR], ws)
        for si in range(5):
            wait_all(RM[si], ms.at[si])
            wait_all(RG[si], gs.at[si])
        wait_all(orecv, osem)
        wait_all(orecv, as_)

    def slots(make):
        return [make(nb) for _, nb in SLOTS]

    dma = pltpu.SemaphoreType.DMA
    scratch = [
        pltpu.VMEM((HL, 576, T), BF16),
        pltpu.VMEM((576, T), BF16),
        pltpu.VMEM((8, T, 576), BF16),
        pltpu.VMEM((8, T, T), BF16),
        pltpu.VMEM((HL, T), F32),
        pltpu.VMEM((nh, TS * JL, T), BF16),
        pltpu.VMEM((T, nh * TS * JL), BF16),
        pltpu.VMEM((nh, JL, T), F32),
        pltpu.VMEM((nh, TS * JL, T), F32),
        pltpu.VMEM((1, T), F32),
        pltpu.VMEM((1, nseq), jnp.int32),
        pltpu.VMEM((nseq, nseq), jnp.int32),
        pltpu.VMEM((8, TS, T), F32),
        pltpu.VMEM((2 * T, T), F32),
        *slots(lambda nb: pltpu.VMEM((T, nb * T), F32)),
        *slots(lambda nb: pltpu.VMEM((PR, TS, nb * T), F32)),
        *slots(lambda nb: pltpu.VMEM((nh, TS * JL, nb * T), F32)),
        *slots(lambda nb: pltpu.VMEM((TS, nb * T), F32)),
        pltpu.VMEM((nh * TS * JL, 2 * T), BF16),
        *slots(lambda nb: pltpu.VMEM((T, nb * T), F32)),
        *slots(lambda nb: pltpu.VMEM((PR, TS, nb * T), F32)),
        *slots(lambda nb: pltpu.VMEM((TS, nb * T), F32)),
        pltpu.VMEM((HOPS - 1, TS, T), F32),
        pltpu.VMEM((T, T), F32),
        dma((9,)), dma((4, 2)), dma((4, 2)), dma((4, 2, 2)), dma((4, 2, 2)), dma((4, 2)), dma((4, 2)),
        dma, dma, dma, dma, dma((5,)), dma((5,)), dma((5,)), dma((5,)), dma, dma, dma, dma,
    ]
    return kernel, scratch


def solution(mesh):
    nseq, nh = mesh.shape["seq"], mesh.shape["head"]
    kernel, scratch = make_kernel(nseq, nh)

    def local(q_main, latent_keys, lse_main, index_queries, index_weights, index_keys, lse_index, slab_order, block_live):
        return pl.pallas_call(
            kernel,
            out_shape=jax.ShapeDtypeStruct(index_keys.shape, F32),
            in_specs=[pl.BlockSpec(memory_space=pltpu.HBM)] * 9,
            out_specs=pl.BlockSpec(memory_space=pltpu.VMEM),
            scratch_shapes=scratch,
            compiler_params=pltpu.CompilerParams(
                collective_id=0, has_side_effects=True, vmem_limit_bytes=60 * 2**20
            ),
        )(
            q_main.transpose(1, 2, 0),
            latent_keys.T,
            lse_main.T,
            index_queries.reshape(-1, index_queries.shape[2]),
            index_weights.T,
            index_keys,
            lse_index.reshape(1, -1),
            slab_order.reshape(1, -1),
            block_live,
        )

    placed = (
        P("seq", "head", None), P("seq", None), P("seq", "head"), P("seq", "head", None), P("seq", "head"),
        P("seq", None), P("seq"), P(), P(),
    )
    return jax.shard_map(local, mesh=mesh, in_specs=placed, out_specs=P("seq", None), check_vma=False)
```

```python
import math

import jax
import jax.numpy as jnp
from jax import lax
from jax.experimental import pallas as pl
from jax.experimental.pallas import tpu as pltpu
from jax.sharding import PartitionSpec as P

HEADS = 128
HOPS = 8
NX = 4

MESH = pl.DeviceIdType.MESH
F32 = jnp.float32
BF16 = jnp.bfloat16
BIG = 3.0e38
MAIN_SCALE = 1.0 / 192.0**0.5
LOG2E = math.log2(math.e)
NT = (((1,), (1,)), ((), ()))


def dot_nt(a, b):
    return lax.dot_general(a, b, NT, preferred_element_type=F32)


def make_kernel(nseq, nh):
    T = 128
    TS = T // nh
    HL = 128 // nh
    JL = 64 // nh
    PR = nh - 1
    C = 576
    HALF, QUART = (C // 2, T // 2), (C // 4, T // 4)
    index_scale = 1.0 / 128.0**0.5
    GH = 4
    FAR_FIRST = sorted(range(1, nh), key=lambda r: -2 * (r // NX) - min(r % NX, NX - r % NX))
    SLOTS = ((0, 1), (1, 2), (3, 2), (5, 2), (7, 1))

    def kernel(
        q_hbm, lat_hbm, lse_hbm, iq_hbm, iw_hbm, ik_hbm, lsei_hbm, order_hbm, blive_hbm,
        out_ref,
        q, qt, kl, ki, lse, iq, iqt, iw, wb, lsei, order, blive, mask, acc,
        m0, m1, m2, m3, m4, r0, r1, r2, r3, r4,
        x0, x1, x2, x3, x4, lg0, lg1, lg2, lg3, lg4, wt,
        g0, g1, g2, g3, g4, h0, h1, h2, h3, h4,
        o0, o1, o2, o3, o4, orecv, fin,
        mb0, mb1, mb2, mb3, mb4, gb0, gb1, gb2, gb3, gb4,
        loc, zs, zr, xs, xr, ds, dr, iqs, iqr, ws, wr, ms, mr, gs, gr, osem, orsem, as_, ar,
    ):
        M = (m0, m1, m2, m3, m4)
        RM = (r0, r1, r2, r3, r4)
        MB = (mb0, mb1, mb2, mb3, mb4)
        GB = (gb0, gb1, gb2, gb3, gb4)
        X = (x0, x1, x2, x3, x4)
        LG = (lg0, lg1, lg2, lg3, lg4)
        G = (g0, g1, g2, g3, g4)
        RG = (h0, h1, h2, h3, h4)
        O = (o0, o1, o2, o3, o4)
        d = lax.axis_index("seq")
        h = lax.axis_index("head")
        c = lax.rem(d, 2)
        x = lax.rem(h, NX)
        yh = h - x
        odd, high = lax.rem(x, 2), x // 2

        def seq(offset):
            return lax.rem(d + offset + nseq, nseq)

        def peer(r):
            return lax.rem(yh + r // NX * NX, nh) + lax.rem(x + r % NX, NX)

        def xpeer(step):
            return yh + lax.rem(x + step, NX)

        barrier = pltpu.get_barrier_semaphore()
        for r in range(1, nh):
            pl.semaphore_signal(barrier, inc=1, device_id=(d, peer(r)), device_id_type=MESH)
        for k in range(1, HOPS):
            pl.semaphore_signal(barrier, inc=1, device_id=(seq(k), h), device_id_type=MESH)
            pl.semaphore_signal(barrier, inc=1, device_id=(seq(-k), h), device_id_type=MESH)

        mine = pl.ds(pl.multiple_of(h * TS, TS), TS)
        my_rows = pl.ds(pl.multiple_of(h * TS * JL, TS * JL), TS * JL)
        locals_ = [
            pltpu.make_async_copy(lat_hbm, kl.at[0], loc.at[0]),
            pltpu.make_async_copy(q_hbm, q, loc.at[1]),
            pltpu.make_async_copy(lse_hbm, lse, loc.at[2]),
            pltpu.make_async_copy(ik_hbm, ki.at[0], loc.at[3]),
            pltpu.make_async_copy(iq_hbm.at[my_rows, :], iq.at[PR], loc.at[4]),
            pltpu.make_async_copy(iw_hbm, iw.at[PR], loc.at[5]),
            pltpu.make_async_copy(lsei_hbm, lsei, loc.at[6]),
            pltpu.make_async_copy(order_hbm, order, loc.at[7]),
            pltpu.make_async_copy(blive_hbm, blive, loc.at[8]),
        ]
        for cp in locals_:
            cp.start()
        pl.semaphore_wait(barrier, PR + 2 * (HOPS - 1))

        def rcopy(src, dst, s, r, dev):
            return pltpu.make_async_remote_copy(
                src_ref=src, dst_ref=dst, send_sem=s, recv_sem=r, device_id=dev, device_id_type=MESH
            )

        def half_at(i, which):
            return pl.ds(pl.multiple_of(HALF[i] * which, HALF[i]), HALF[i])

        own_half = [half_at(i, odd) for i in range(2)]
        other_half = [half_at(i, 1 - odd) for i in range(2)]
        own_quart = [pl.ds(pl.multiple_of(HALF[i] * odd + QUART[i] * high, QUART[i]), QUART[i]) for i in range(2)]
        whole = [pl.ds(0, C), pl.ds(0, T)]
        keys_at = (kl, ki)

        def pieces(src, block, rows, s, r, dev):
            return [
                rcopy(src[i].at[rows[i], :], keys_at[i].at[block, rows[i], :], s.at[i], r.at[i], dev)
                for i in range(2)
            ]

        def kpieces(block, rows, s, r, dev):
            return pieces((kl.at[block], ki.at[block]), block, rows, s, r, dev)

        own_keys = (lat_hbm, ik_hbm)

        def zcopies(j):
            if j < 4:
                return pieces(own_keys, 2 * j - 1 + c, own_half, zs.at[j - 1], zr.at[j - 1], (seq(2 * j), h))
            return pieces(own_keys, 7, own_half, zs.at[3], zr.at[3], (seq(7), h))

        def own_to_partner():
            return pieces(own_keys, 7, whole, ds.at[3, 0], dr.at[3, 0], (seq(1), h))

        def send_index(rs):
            for r in rs:
                to = peer(r)
                rows = pl.ds(pl.multiple_of(to * TS * JL, TS * JL), TS * JL)
                rcopy(iq_hbm.at[rows, :], iq.at[r - 1], iqs, iqr, (d, to)).start()
                rcopy(iw_hbm, iw.at[r - 1], ws, wr, (d, to)).start()

        def far_sends():
            for cp in zcopies(3):
                cp.start()

            @pl.when(c == 1)
            def _():
                for cp in zcopies(4):
                    cp.start()

            @pl.when(c == 0)
            def _():
                for cp in own_to_partner():
                    cp.start()

        send_index(range(1, NX))
        for j in (1, 2):
            for cp in zcopies(j):
                cp.start()

        for cp in locals_:
            cp.wait()

        @pl.loop(0, HL // 4)
        def _(i):
            for u in range(4):
                a = i * 4 + u
                v = lse[pl.ds(a, 1), :] * (-1.0 / MAIN_SCALE)
                hi = v.astype(BF16).astype(F32)
                mid = (v - hi).astype(BF16).astype(F32)
                low = v - hi - mid
                row = lax.broadcasted_iota(jnp.int32, (64, T), 0)
                ext = jnp.where(row == 0, hi, jnp.where(row == 1, mid, jnp.where(row == 2, low, 0.0)))
                qt[a] = jnp.concatenate([q[a], ext.astype(BF16)], axis=0).T

        far_sends()

        lane64 = lax.broadcasted_iota(jnp.int32, (1, nseq), 1)
        order_f = order[...].astype(F32)

        def entry(at):
            return jnp.sum(jnp.where(lane64 == at, order_f, 0.0), axis=1, keepdims=True)

        own_slab = entry(d)
        row64 = lax.broadcasted_iota(jnp.int32, (nseq, nseq), 0).astype(F32)
        live_row = jnp.sum(jnp.where(row64 == own_slab, blive[...].astype(F32), 0.0), axis=0, keepdims=True)
        lane64f = lane64.astype(F32)
        t_at = (h * TS + lax.broadcasted_iota(jnp.int32, (TS, T), 0)).astype(F32) + own_slab * T
        s_in = lax.broadcasted_iota(jnp.int32, (TS, T), 1).astype(F32)
        hops = [0 * c] + [2 * j + c - cc for j in (1, 2, 3) for cc in (0, 1)] + [7 - 6 * c]
        for b in range(8):
            slab = entry(seq(-hops[b]))
            allowed = jnp.sum(jnp.where(lane64f == slab, live_row, 0.0), axis=1, keepdims=True)
            mask[b] = jnp.where((s_in + slab * T <= t_at) & (allowed == 1.0), 1.0, 0.0)
        lane_t = lax.broadcasted_iota(jnp.int32, (TS, T), 1)
        row_t = h * TS + lax.broadcasted_iota(jnp.int32, (TS, T), 0)
        lse_col = jnp.sum(jnp.where(lane_t == row_t, lsei[...], 0.0), axis=1, keepdims=True)

        def side_by_side(vs):
            return jnp.concatenate(vs, axis=1) if len(vs) > 1 else vs[0]

        def mass(si):
            b0, nb = SLOTS[si]
            ones = jnp.where(lax.broadcasted_iota(jnp.int32, (64, nb * T), 0) < 3, 1.0, 0.0).astype(BF16)
            keys = jnp.concatenate([side_by_side([kl[b0 + b] for b in range(nb)]), ones], axis=0)
            part = None
            for u in range(HL // GH):
                heads = qt[u * GH : (u + 1) * GH].reshape(GH * T, C + 64)
                e = jnp.exp2(jnp.dot(heads, keys, preferred_element_type=F32) * (MAIN_SCALE * LOG2E))
                for v in range(GH):
                    ev = e[v * T : (v + 1) * T]
                    part = ev if part is None else part + ev
            M[si][...] = part
            MB[si][...] = M[si][...].astype(BF16)
            for r in FAR_FIRST:
                to = peer(r)
                toks = pl.ds(pl.multiple_of(to * TS, TS), TS)
                rcopy(MB[si].at[toks, :], RM[si].at[r - 1], ms.at[si], mr.at[si], (d, to)).start()

        def wait_all(ref, sem):
            pltpu.make_async_copy(ref, ref, sem).wait()

        def wait_recv(copies):
            for cp in copies:
                cp.wait_recv()

        def block_of(j):
            return 2 * j - 1 + c if j < 4 else 7

        def x_copies(j, way):
            return kpieces(
                block_of(j), own_quart, xs.at[j - 1, way], xr.at[j - 1, way], (d, xpeer((1, NX - 1)[way]))
            )

        def d_copies(j, part):
            rows = (own_half, other_half)[part]
            return kpieces(2 * j - 1 + c, rows, ds.at[j - 1, part], dr.at[j - 1, part], (d + 1 - 2 * c, h))

        def relay_z(j):
            wait_recv(kpieces(block_of(j), own_half, zs.at[j - 1], zr.at[j - 1], (d, h)))
            for way in (0, 1):
                for cp in x_copies(j, way):
                    cp.start()
            if j < 4:
                for cp in d_copies(j, 0):
                    cp.start()

        def x_arrived(j):
            for way in (0, 1):
                wait_recv(x_copies(j, way))

        def relay_x(j):
            x_arrived(j)
            for cp in d_copies(j, 1):
                cp.start()

        def wait_d(j):
            for part in (0, 1):
                rows = (own_half, other_half)[part]
                wait_recv(kpieces(2 * j - c, rows, ds.at[j - 1, part], dr.at[j - 1, part], (d, h)))

        def index_tables():
            wait_all(iq.at[0:PR], iqr)
            wait_all(iw.at[0:PR], wr)
            eye = jnp.where(
                lax.broadcasted_iota(jnp.int32, (T, T), 0) == lax.broadcasted_iota(jnp.int32, (T, T), 1), 1.0, 0.0
            ).astype(BF16)
            pick = lax.broadcasted_iota(jnp.int32, (TS, JL, T), 0) + h * TS == lax.broadcasted_iota(jnp.int32, (TS, JL, T), 2)
            for hh in range(nh):
                iqt[:, hh * T : (hh + 1) * T] = dot_nt(eye, iq[hh]).astype(BF16)
                w = jnp.broadcast_to(iw[hh][None], (TS, JL, T))
                col = jnp.sum(jnp.where(pick, w, 0.0), axis=2, keepdims=True).reshape(TS * JL, 1)
                wb[hh] = jnp.broadcast_to(col, (TS * JL, T))

        def phase_a(si):
            b0, nb = SLOTS[si]
            keys = ki[b0 : b0 + nb].reshape(nb * T, T)
            part = None
            for hh in range(nh):
                xv = dot_nt(iq[hh], keys)
                wm = jnp.where(xv > 0.0, side_by_side([wb[hh]] * nb), 0.0)
                X[si][hh] = wm
                part = xv * wm if part is None else part + xv * wm
            LG[si][...] = jnp.sum(part.reshape(TS, JL, nb * T), axis=1)

        def phase_b(si):
            b0, nb = SLOTS[si]
            wait_all(RM[si], mr.at[si])
            total = M[si][mine, :]
            for r in range(PR):
                total = total + RM[si][r].astype(F32)
            live = side_by_side([mask[b0 + b] for b in range(nb)])
            g = jnp.where(live > 0.0, jnp.exp(LG[si][...] * index_scale - lse_col) - total * (1.0 / HEADS), 0.0)
            g = jnp.clip(g, -BIG, BIG)
            gv = jnp.broadcast_to(g[:, None, :], (TS, JL, nb * T)).reshape(TS * JL, nb * T)
            ac = acc.at[:, 0 : nb * T]
            ac[...] = gv

            @pl.loop(0, nh // 4)
            def _(i):
                for u in range(4):
                    hh = i * 4 + u
                    rows = pl.ds(pl.multiple_of(hh * TS * JL, TS * JL), TS * JL)
                    wt[rows, 0 : nb * T] = (ac[...] * X[si][hh]).astype(BF16)

            G[si][...] = jnp.dot(iqt[...], wt[:, 0 : nb * T], preferred_element_type=F32)
            GB[si][...] = G[si][...].astype(BF16)
            for r in FAR_FIRST:
                to = peer(r)
                toks = pl.ds(pl.multiple_of(to * TS, TS), TS)
                rcopy(GB[si].at[toks, :], RG[si].at[r - 1], gs.at[si], gr.at[si], (d, to)).start()

        def phase_c(si):
            b0, nb = SLOTS[si]
            wait_all(RG[si], gr.at[si])
            total = G[si][mine, :]
            for r in range(PR):
                total = total + RG[si][r].astype(F32)
            O[si][...] = total
            if si > 0:
                for b in range(nb):
                    k = hops[b0 + b]
                    rcopy(
                        O[si].at[:, b * T : (b + 1) * T], orecv.at[k - 1], osem, orsem, (seq(-k), h)
                    ).start()

        mass(0)
        relay_z(1)
        relay_z(2)
        relay_x(1)
        relay_z(3)
        relay_x(2)
        wait_d(1)
        mass(1)

        @pl.when(c == 0)
        def _():
            relay_z(4)

        send_index(range(NX, nh))
        relay_x(3)
        wait_d(2)
        mass(2)
        wait_d(3)
        mass(3)

        @pl.when(c == 0)
        def _():
            x_arrived(4)

        @pl.when(c == 1)
        def _():
            wait_recv(own_to_partner())

        mass(4)
        index_tables()
        phase_a(0)
        phase_b(0)
        phase_a(1)
        phase_b(1)
        phase_a(2)
        phase_b(2)
        phase_a(3)
        phase_a(4)
        phase_b(3)
        phase_b(4)
        phase_c(0)
        phase_c(1)
        phase_c(2)
        phase_c(3)
        phase_c(4)

        wait_all(orecv, orsem)
        total = O[0][...]
        for k in range(HOPS - 1):
            total = total + orecv[k]
        fin[mine, :] = total * index_scale
        for r in FAR_FIRST:
            rcopy(fin.at[mine, :], fin.at[mine, :], as_, ar, (d, peer(r))).start()
        wait_all(fin.at[0 : PR * TS, :], ar)
        out_ref[...] = fin[...].T

        for j in (1, 2, 3):
            for cp in zcopies(j) + x_copies(j, 0) + x_copies(j, 1) + d_copies(j, 0) + d_copies(j, 1):
                cp.wait_send()

        @pl.when(c == 1)
        def _():
            for cp in zcopies(4):
                cp.wait_send()

        @pl.when(c == 0)
        def _():
            for cp in own_to_partner() + x_copies(4, 0) + x_copies(4, 1):
                cp.wait_send()

        wait_all(iq.at[0:PR], iqs)
        wait_all(iw.at[0:PR], ws)
        for si in range(5):
            wait_all(RM[si], ms.at[si])
            wait_all(RG[si], gs.at[si])
        wait_all(orecv, osem)
        wait_all(fin.at[0 : PR * TS, :], as_)

    def slots(make):
        return [make(nb) for _, nb in SLOTS]

    dma = pltpu.SemaphoreType.DMA
    scratch = [
        pltpu.VMEM((HL, C, T), BF16),
        pltpu.VMEM((HL, T, C + 64), BF16),
        pltpu.VMEM((8, C, T), BF16),
        pltpu.VMEM((8, T, T), BF16),
        pltpu.VMEM((HL, T), F32),
        pltpu.VMEM((nh, TS * JL, T), BF16),
        pltpu.VMEM((T, nh * TS * JL), BF16),
        pltpu.VMEM((nh, JL, T), F32),
        pltpu.VMEM((nh, TS * JL, T), F32),
        pltpu.VMEM((1, T), F32),
        pltpu.VMEM((1, nseq), jnp.int32),
        pltpu.VMEM((nseq, nseq), jnp.int32),
        pltpu.VMEM((8, TS, T), F32),
        pltpu.VMEM((TS * JL, 2 * T), F32),
        *slots(lambda nb: pltpu.VMEM((T, nb * T), F32)),
        *slots(lambda nb: pltpu.VMEM((PR, TS, nb * T), BF16)),
        *slots(lambda nb: pltpu.VMEM((nh, TS * JL, nb * T), F32)),
        *slots(lambda nb: pltpu.VMEM((TS, nb * T), F32)),
        pltpu.VMEM((nh * TS * JL, 2 * T), BF16),
        *slots(lambda nb: pltpu.VMEM((T, nb * T), F32)),
        *slots(lambda nb: pltpu.VMEM((PR, TS, nb * T), BF16)),
        *slots(lambda nb: pltpu.VMEM((TS, nb * T), F32)),
        pltpu.VMEM((HOPS - 1, TS, T), F32),
        pltpu.VMEM((T, T), F32),
        *slots(lambda nb: pltpu.VMEM((T, nb * T), BF16)),
        *slots(lambda nb: pltpu.VMEM((T, nb * T), BF16)),
        dma((9,)), dma((4, 2)), dma((4, 2)), dma((4, 2, 2)), dma((4, 2, 2)), dma((4, 2, 2)), dma((4, 2, 2)),
        dma, dma, dma, dma, dma((5,)), dma((5,)), dma((5,)), dma((5,)), dma, dma, dma, dma,
    ]
    return kernel, scratch


def solution(mesh):
    nseq, nh = mesh.shape["seq"], mesh.shape["head"]
    kernel, scratch = make_kernel(nseq, nh)

    def local(q_main, latent_keys, lse_main, index_queries, index_weights, index_keys, lse_index, slab_order, block_live):
        return pl.pallas_call(
            kernel,
            out_shape=pltpu.VMEM(index_keys.shape, F32),
            in_specs=[pl.BlockSpec(memory_space=pltpu.HBM)] * 9,
            out_specs=pl.BlockSpec(memory_space=pltpu.VMEM),
            scratch_shapes=scratch,
            compiler_params=pltpu.CompilerParams(
                collective_id=0, has_side_effects=True, vmem_limit_bytes=60 * 2**20
            ),
        )(
            q_main.transpose(1, 2, 0),
            latent_keys.T,
            lse_main.T,
            index_queries.reshape(-1, index_queries.shape[2]),
            index_weights.T,
            index_keys,
            lse_index.reshape(1, -1),
            slab_order.reshape(1, -1),
            block_live,
        )

    placed = (
        P("seq", "head", None), P("seq", None), P("seq", "head"), P("seq", "head", None), P("seq", "head"),
        P("seq", None), P("seq"), P(), P(),
    )
    return jax.shard_map(local, mesh=mesh, in_specs=placed, out_specs=P("seq", None), check_vma=False)
```

```python
import math

import jax
import jax.numpy as jnp
from jax import lax
from jax.experimental import pallas as pl
from jax.experimental.pallas import tpu as pltpu
from jax.sharding import PartitionSpec as P

HEADS = 128
HOPS = 8
NX = 4

MESH = pl.DeviceIdType.MESH
F32 = jnp.float32
BF16 = jnp.bfloat16
BIG = 3.0e38
MAIN_SCALE = 1.0 / 192.0**0.5
LOG2E = math.log2(math.e)
NT = (((1,), (1,)), ((), ()))


def dot_nt(a, b):
    return lax.dot_general(a, b, NT, preferred_element_type=F32)


def make_kernel(nseq, nh):
    T = 128
    TS = T // nh
    HL = 128 // nh
    JL = 64 // nh
    PR = nh - 1
    C = 576
    HALF, QUART = (C // 2, T // 2), (C // 4, T // 4)
    index_scale = 1.0 / 128.0**0.5
    GH = 4
    HROWS = C // 2 + T // 2
    LROWS = 2 * HL + TS * JL + 2 * JL
    FAR_FIRST = sorted(range(1, nh), key=lambda r: -2 * (r // NX) - min(r % NX, NX - r % NX))
    SLOTS = ((0, 1), (1, 2), (3, 2), (5, 2), (7, 1))

    def kernel(
        q_hbm, lat_hbm, lse_hbm, iq_hbm, iw_hbm, ik_hbm, lsei_hbm, order_hbm, blive_hbm,
        out_ref,
        q, qt, kl, ki, lse, iq, iqt, iw, wb, lsei, order, blive, mask, acc,
        m0, m1, m2, m3, m4, r0, r1, r2, r3, r4,
        x0, x1, x2, x3, x4, lg0, lg1, lg2, lg3, lg4, wt,
        g0, g1, g2, g3, g4, h0, h1, h2, h3, h4,
        o0, o1, o2, o3, o4, orecv, fin,
        mb0, mb1, mb2, mb3, mb4, gb0, gb1, gb2, gb3, gb4,
        loc, ks, zr, xr, dr, iqr, ws, wr, ms, mr, gr, osem, orsem, as_, ar,
    ):
        M = (m0, m1, m2, m3, m4)
        RM = (r0, r1, r2, r3, r4)
        MB = (mb0, mb1, mb2, mb3, mb4)
        GB = (gb0, gb1, gb2, gb3, gb4)
        X = (x0, x1, x2, x3, x4)
        LG = (lg0, lg1, lg2, lg3, lg4)
        G = (g0, g1, g2, g3, g4)
        RG = (h0, h1, h2, h3, h4)
        O = (o0, o1, o2, o3, o4)
        d = lax.axis_index("seq")
        h = lax.axis_index("head")
        c = lax.rem(d, 2)
        x = lax.rem(h, NX)
        yh = h - x
        odd, high = lax.rem(x, 2), x // 2

        def wait_all(ref, sem):
            pltpu.make_async_copy(ref, ref, sem).wait()

        def seq(offset):
            return lax.rem(d + offset + nseq, nseq)

        def peer(r):
            return lax.rem(yh + r // NX * NX, nh) + lax.rem(x + r % NX, NX)

        def xpeer(step):
            return yh + lax.rem(x + step, NX)

        mine = pl.ds(pl.multiple_of(h * TS, TS), TS)
        my_rows = pl.ds(pl.multiple_of(h * TS * JL, TS * JL), TS * JL)
        locals_ = [
            pltpu.make_async_copy(lat_hbm, kl.at[0], loc.at[0]),
            pltpu.make_async_copy(q_hbm, q, loc.at[1]),
            pltpu.make_async_copy(lse_hbm, lse, loc.at[2]),
            pltpu.make_async_copy(ik_hbm, ki.at[0], loc.at[0]),
            pltpu.make_async_copy(iq_hbm.at[my_rows, :], iq.at[PR], loc.at[2]),
            pltpu.make_async_copy(iw_hbm, iw.at[PR], loc.at[2]),
            pltpu.make_async_copy(lsei_hbm, lsei, loc.at[3]),
            pltpu.make_async_copy(order_hbm, order, loc.at[4]),
            pltpu.make_async_copy(blive_hbm, blive, loc.at[5]),
        ]
        barrier = pltpu.get_barrier_semaphore()
        for r in FAR_FIRST:
            pl.semaphore_signal(barrier, inc=1, device_id=(d, peer(r)), device_id_type=MESH)
        for k in range(HOPS - 1, 0, -1):
            pl.semaphore_signal(barrier, inc=1, device_id=(seq(k), h), device_id_type=MESH)
            pl.semaphore_signal(barrier, inc=1, device_id=(seq(-k), h), device_id_type=MESH)
        for k in (-2, 2):
            for step in (1, NX - 1):
                pl.semaphore_signal(barrier, inc=1, device_id=(seq(k), xpeer(step)), device_id_type=MESH)

        locals_[0].start()
        locals_[3].start()

        for i in (1, 2, 4, 5, 6, 7, 8):
            locals_[i].start()
        wait_all(kl.at[0:2, 0:HROWS, :], loc.at[0])
        pl.semaphore_wait(barrier, PR + 2 * (HOPS - 1) + 4)

        def rcopy(src, dst, s, r, dev):
            return pltpu.make_async_remote_copy(
                src_ref=src, dst_ref=dst, send_sem=s, recv_sem=r, device_id=dev, device_id_type=MESH
            )

        def half_at(i, which):
            return pl.ds(pl.multiple_of(HALF[i] * which, HALF[i]), HALF[i])

        own_half = [half_at(i, odd) for i in range(2)]
        other_half = [half_at(i, 1 - odd) for i in range(2)]
        own_quart = [pl.ds(pl.multiple_of(HALF[i] * odd + QUART[i] * high, QUART[i]), QUART[i]) for i in range(2)]
        whole = [pl.ds(0, C), pl.ds(0, T)]
        keys_at = (kl, ki)

        def pieces(src, block, rows, r, dev):
            return [
                rcopy(src[i].at[rows[i], :], keys_at[i].at[block, rows[i], :], ks, r, dev)
                for i in range(2)
            ]

        def kpieces(block, rows, r, dev):
            return pieces((kl.at[block], ki.at[block]), block, rows, r, dev)

        own_keys = (kl.at[0], ki.at[0])

        second = (kl.at[3 + c], ki.at[3 + c])

        def zcopies(j):
            return pieces(own_keys, 2 * j - 1 + c, own_half, zr.at[j - 1], (seq(2 * j), h))

        def third_relay():
            return pieces(second, 5 + c, own_half, zr.at[2], (seq(2), h))

        def third_quarters(way):
            return pieces(
                second, 5 + c, own_quart, xr.at[2], (seq(2), xpeer((1, NX - 1)[way]))
            )

        def fourth_relay():
            return pieces(second, 7, own_half, zr.at[3], (seq(3), h))

        def own_to_partner():
            return pieces(own_keys, 7, whole, dr.at[3], (seq(1), h))

        def send_index(rs):
            for r in rs:
                to = peer(r)
                rows = pl.ds(pl.multiple_of(to * TS * JL, TS * JL), TS * JL)
                rcopy(iq_hbm.at[rows, :], iq.at[r - 1], ms, iqr, (d, to)).start()
                rcopy(iw_hbm, iw.at[r - 1], ws, wr, (d, to)).start()

        def far_sends():
            @pl.when(c == 0)
            def _():
                for cp in own_to_partner():
                    cp.start()

        send_index(range(1, NX))
        for j in (2, 1):
            for cp in zcopies(j):
                cp.start()

        for i in (1, 6, 7, 8):
            locals_[i].wait()
        wait_all(kl.at[0, 0:LROWS, :], loc.at[2])

        @pl.loop(0, HL // 4)
        def _(i):
            for u in range(4):
                a = i * 4 + u
                v = lse[pl.ds(a, 1), :] * (-1.0 / MAIN_SCALE)
                hi = v.astype(BF16).astype(F32)
                mid = (v - hi).astype(BF16).astype(F32)
                low = v - hi - mid
                row = lax.broadcasted_iota(jnp.int32, (64, T), 0)
                ext = jnp.where(row == 0, hi, jnp.where(row == 1, mid, jnp.where(row == 2, low, 0.0)))
                qt[a] = jnp.concatenate([q[a], ext.astype(BF16)], axis=0).T

        far_sends()

        lane64 = lax.broadcasted_iota(jnp.int32, (1, nseq), 1)
        order_f = order[...].astype(F32)

        def entry(at):
            return jnp.sum(jnp.where(lane64 == at, order_f, 0.0), axis=1, keepdims=True)

        own_slab = entry(d)
        row64 = lax.broadcasted_iota(jnp.int32, (nseq, nseq), 0).astype(F32)
        live_row = jnp.sum(jnp.where(row64 == own_slab, blive[...].astype(F32), 0.0), axis=0, keepdims=True)
        lane64f = lane64.astype(F32)
        t_at = (h * TS + lax.broadcasted_iota(jnp.int32, (TS, T), 0)).astype(F32) + own_slab * T
        s_in = lax.broadcasted_iota(jnp.int32, (TS, T), 1).astype(F32)
        hops = [0 * c] + [2 * j + c - cc for j in (1, 2, 3) for cc in (0, 1)] + [7 - 6 * c]
        for b in range(8):
            slab = entry(seq(-hops[b]))
            allowed = jnp.sum(jnp.where(lane64f == slab, live_row, 0.0), axis=1, keepdims=True)
            mask[b] = jnp.where((s_in + slab * T <= t_at) & (allowed == 1.0), 1.0, 0.0)
        lane_t = lax.broadcasted_iota(jnp.int32, (TS, T), 1)
        row_t = h * TS + lax.broadcasted_iota(jnp.int32, (TS, T), 0)
        lse_col = jnp.sum(jnp.where(lane_t == row_t, lsei[...], 0.0), axis=1, keepdims=True)

        def side_by_side(vs):
            return jnp.concatenate(vs, axis=1) if len(vs) > 1 else vs[0]

        def mass(si):
            b0, nb = SLOTS[si]
            ones = jnp.where(lax.broadcasted_iota(jnp.int32, (64, nb * T), 0) < 3, 1.0, 0.0).astype(BF16)
            keys = jnp.concatenate([side_by_side([kl[b0 + b] for b in range(nb)]), ones], axis=0)
            part = None
            for u in range(HL // GH):
                heads = qt[u * GH : (u + 1) * GH].reshape(GH * T, C + 64)
                e = jnp.exp2(jnp.dot(heads, keys, preferred_element_type=F32) * (MAIN_SCALE * LOG2E))
                for v in range(GH):
                    ev = e[v * T : (v + 1) * T]
                    part = ev if part is None else part + ev
            M[si][...] = part
            MB[si][...] = M[si][...].astype(BF16)
            for r in FAR_FIRST:
                to = peer(r)
                toks = pl.ds(pl.multiple_of(to * TS, TS), TS)
                rcopy(MB[si].at[toks, :], RM[si].at[r - 1], ms, mr.at[si], (d, to)).start()

        def block_of(j):
            return 2 * j - 1 + c if j < 4 else 7

        def x_copies(j, way):
            return kpieces(
                block_of(j), own_quart, xr.at[j - 1], (d, xpeer((1, NX - 1)[way]))
            )

        def d_copies(j, part):
            rows = (own_half, other_half)[part]
            return kpieces(2 * j - 1 + c, rows, dr.at[j - 1], (d + 1 - 2 * c, h))

        def relay_z(j):
            wait_all(kl.at[0, 0:HROWS, :], zr.at[j - 1])
            if j == 2:
                for cp in third_relay() + third_quarters(0) + third_quarters(1):
                    cp.start()

                @pl.when(c == 1)
                def _():
                    for cp in fourth_relay():
                        cp.start()

            if j != 3:
                for way in (0, 1):
                    for cp in x_copies(j, way):
                        cp.start()
            if j < 4:
                for cp in d_copies(j, 0):
                    cp.start()

        def x_arrived(j):
            wait_all(kl.at[0, 0:HROWS, :], xr.at[j - 1])

        def relay_x(j):
            x_arrived(j)
            for cp in d_copies(j, 1):
                cp.start()

        def wait_d(j):
            wait_all(kl.at[0:2, 0:HROWS, :], dr.at[j - 1])

        def index_tables():
            wait_all(iq.at[0:PR], iqr)
            wait_all(iw.at[0:PR], wr)
            eye = jnp.where(
                lax.broadcasted_iota(jnp.int32, (T, T), 0) == lax.broadcasted_iota(jnp.int32, (T, T), 1), 1.0, 0.0
            ).astype(BF16)
            pick = lax.broadcasted_iota(jnp.int32, (TS, JL, T), 0) + h * TS == lax.broadcasted_iota(jnp.int32, (TS, JL, T), 2)
            for hh in range(nh):
                iqt[:, hh * T : (hh + 1) * T] = dot_nt(eye, iq[hh]).astype(BF16)
                w = jnp.broadcast_to(iw[hh][None], (TS, JL, T))
                col = jnp.sum(jnp.where(pick, w, 0.0), axis=2, keepdims=True).reshape(TS * JL, 1)
                wb[hh] = jnp.broadcast_to(col, (TS * JL, T))

        def phase_a(si):
            b0, nb = SLOTS[si]
            keys = ki[b0 : b0 + nb].reshape(nb * T, T)
            part = None
            for hh in range(nh):
                xv = dot_nt(iq[hh], keys)
                wm = jnp.where(xv > 0.0, side_by_side([wb[hh]] * nb), 0.0)
                X[si][hh] = wm
                part = xv * wm if part is None else part + xv * wm
            LG[si][...] = jnp.sum(part.reshape(TS, JL, nb * T), axis=1)

        def phase_b(si):
            b0, nb = SLOTS[si]
            wait_all(RM[si], mr.at[si])
            total = M[si][mine, :]
            for r in range(PR):
                total = total + RM[si][r].astype(F32)
            live = side_by_side([mask[b0 + b] for b in range(nb)])
            g = jnp.where(live > 0.0, jnp.exp(LG[si][...] * index_scale - lse_col) - total * (1.0 / HEADS), 0.0)
            g = jnp.clip(g, -BIG, BIG)
            gv = jnp.broadcast_to(g[:, None, :], (TS, JL, nb * T)).reshape(TS * JL, nb * T)
            for hh in range(nh):
                wt[hh * TS * JL : (hh + 1) * TS * JL, 0 : nb * T] = (gv * X[si][hh]).astype(BF16)

            G[si][...] = jnp.dot(iqt[...], wt[:, 0 : nb * T], preferred_element_type=F32)
            GB[si][...] = G[si][...].astype(BF16)
            for r in FAR_FIRST:
                to = peer(r)
                toks = pl.ds(pl.multiple_of(to * TS, TS), TS)
                rcopy(GB[si].at[toks, :], RG[si].at[r - 1], ms, gr.at[si], (d, to)).start()

        def phase_c(si):
            b0, nb = SLOTS[si]
            wait_all(RG[si], gr.at[si])
            total = G[si][mine, :]
            for r in range(PR):
                total = total + RG[si][r].astype(F32)
            O[si][...] = total
            if si > 0:
                for b in range(nb):
                    k = hops[b0 + b]
                    rcopy(
                        O[si].at[:, b * T : (b + 1) * T], orecv.at[k - 1], osem, orsem, (seq(-k), h)
                    ).start()

        mass(0)
        relay_z(2)
        relay_z(1)
        relay_x(2)
        send_index(reversed(range(NX, nh)))
        relay_x(1)

        @pl.when(c == 0)
        def _():
            relay_z(4)

        wait_d(2)
        mass(2)
        relay_z(3)
        relay_x(3)
        wait_d(1)
        mass(1)
        wait_d(3)
        mass(3)

        @pl.when(c == 0)
        def _():
            x_arrived(4)

        @pl.when(c == 1)
        def _():
            wait_d(4)

        mass(4)
        index_tables()
        phase_a(2)
        phase_b(2)
        phase_a(1)
        phase_b(1)
        phase_a(3)
        phase_b(3)
        phase_a(4)
        phase_b(4)
        phase_a(0)
        phase_b(0)
        phase_c(2)
        phase_c(1)
        phase_c(3)
        phase_c(4)
        phase_c(0)

        wait_all(orecv, orsem)
        total = O[0][...]
        for k in range(HOPS - 1):
            total = total + orecv[k]
        fin[mine, :] = total * index_scale
        for r in FAR_FIRST:
            rcopy(fin.at[mine, :], fin.at[mine, :], as_, ar, (d, peer(r))).start()
        @pl.when(c == 0)
        def _():
            wait_all(q.at[0:15, 0:HROWS, :], ks)

        @pl.when(c == 1)
        def _():
            wait_all(q.at[0:13, 0:HROWS, :], ks)

        wait_all(q.at[0:14, 0 : PR * (T + 2 * T) // 14, :], ms)
        wait_all(iw.at[0:PR], ws)
        wait_all(orecv, osem)

        wait_all(fin.at[0 : PR * TS, :], ar)
        out_ref[...] = fin[...].T
        wait_all(fin.at[0 : PR * TS, :], as_)

    def slots(make):
        return [make(nb) for _, nb in SLOTS]

    dma = pltpu.SemaphoreType.DMA
    scratch = [
        pltpu.VMEM((HL, C, T), BF16),
        pltpu.VMEM((HL, T, C + 64), BF16),
        pltpu.VMEM((8, C, T), BF16),
        pltpu.VMEM((8, T, T), BF16),
        pltpu.VMEM((HL, T), F32),
        pltpu.VMEM((nh, TS * JL, T), BF16),
        pltpu.VMEM((T, nh * TS * JL), BF16),
        pltpu.VMEM((nh, JL, T), F32),
        pltpu.VMEM((nh, TS * JL, T), F32),
        pltpu.VMEM((1, T), F32),
        pltpu.VMEM((1, nseq), jnp.int32),
        pltpu.VMEM((nseq, nseq), jnp.int32),
        pltpu.VMEM((8, TS, T), F32),
        pltpu.VMEM((TS * JL, 2 * T), F32),
        *slots(lambda nb: pltpu.VMEM((T, nb * T), F32)),
        *slots(lambda nb: pltpu.VMEM((PR, TS, nb * T), BF16)),
        *slots(lambda nb: pltpu.VMEM((nh, TS * JL, nb * T), F32)),
        *slots(lambda nb: pltpu.VMEM((TS, nb * T), F32)),
        pltpu.VMEM((nh * TS * JL, 2 * T), BF16),
        *slots(lambda nb: pltpu.VMEM((T, nb * T), F32)),
        *slots(lambda nb: pltpu.VMEM((PR, TS, nb * T), BF16)),
        *slots(lambda nb: pltpu.VMEM((TS, nb * T), F32)),
        pltpu.VMEM((HOPS - 1, TS, T), F32),
        pltpu.VMEM((T, T), F32),
        *slots(lambda nb: pltpu.VMEM((T, nb * T), BF16)),
        *slots(lambda nb: pltpu.VMEM((T, nb * T), BF16)),
        dma((6,)), dma, dma((4,)), dma((4,)), dma((4,)),
        dma, dma, dma, dma, dma((5,)), dma((5,)), dma, dma, dma, dma,
    ]
    return kernel, scratch


def solution(mesh):
    nseq, nh = mesh.shape["seq"], mesh.shape["head"]
    kernel, scratch = make_kernel(nseq, nh)

    def local(q_main, latent_keys, lse_main, index_queries, index_weights, index_keys, lse_index, slab_order, block_live):
        return pl.pallas_call(
            kernel,
            out_shape=pltpu.VMEM(index_keys.shape, F32),
            in_specs=[pl.BlockSpec(memory_space=pltpu.HBM)] * 9,
            out_specs=pl.BlockSpec(memory_space=pltpu.VMEM),
            scratch_shapes=scratch,
            compiler_params=pltpu.CompilerParams(
                collective_id=0, has_side_effects=True, vmem_limit_bytes=60 * 2**20
            ),
        )(
            q_main.transpose(1, 2, 0),
            latent_keys.T,
            lse_main.T,
            index_queries.reshape(-1, index_queries.shape[2]),
            index_weights.T,
            index_keys,
            lse_index.reshape(1, -1),
            slab_order.reshape(1, -1),
            block_live,
        )

    placed = (
        P("seq", "head", None), P("seq", None), P("seq", "head"), P("seq", "head", None), P("seq", "head"),
        P("seq", None), P("seq"), P(), P(),
    )
    return jax.shard_map(local, mesh=mesh, in_specs=placed, out_specs=P("seq", None), check_vma=False)
```
